32 devices in a mesh: patch: 16 (over z, y, x), sub: 2 (over core).
Axes of the slice: x: 2, y: 2, z: 4, core: 2. Of those that a mesh axis runs over, the one named last changes fastest.
Arguments:
- fields: float32 [5, 64, 128, 128], P(None, ('patch', 'sub')), may hold values from -6 to 6
- density: float32 [64, 128, 128], P(('patch', 'sub')), may hold values from 1 to 3
- moduli: float32 [2, 64, 128, 128], P(None, ('patch', 'sub')), may hold values from 0.5 to 128
- metric_diag: float32 [2, 64, 128, 128], P(None, ('patch', 'sub')), may hold values from 0.7 to 1.3
- metric_cross: float32 [2, 64, 128, 128], P(None, ('patch', 'sub')), may hold values from -0.3 to 0.3
- fc_extension: float32 [25, 10], replicated, may hold values from -2 to 2
- patch_count: int32 [32], P(('patch', 'sub')), may hold values from 1 to 2, as said below
- connectivity: int32 [256, 3], P(('patch', 'sub')), may hold values from -1 to 31, as said below
Outputs:
- advanced: float32 [5, 64, 128, 128], P(None, ('patch', 'sub'))
The draws below stay inside these ranges and needn't reach their ends.
Inputs may be any that keep to these rules, and one draw needn't show every extreme that they name: `patch_count`: every device holds at most 2 live patches; the largest count is 2 in every draw. `connectivity`: links join only live slots and are symmetric with equal orientation flags on both ends; a neighbour is held by the same device or by the device whose flat index differs by 1 or 17 modulo 32; from one device to another device go at most 2 linked sides, and this number is reached in every draw.
All inputs are finite; a program needn't handle non-finite values.
Results may differ from the reference program's by a relative error of at most 0.00005.
Values sent between devices are 32-bit elements; how exact they have to be, the bound alone decides.
A program may use at most 64 MiB of HBM per device.

```python
import math
import jax
import jax.numpy as jnp
from jax import lax

N = 128
CONT = 25
MATCH = 5
PMAX = 2
STRIDE = 17
SLOTS = 64
DEVICES = 32


def patch_layout(key):
    base = jax.random.fold_in(key, 11)
    key_count, key_west, key_north = jax.random.split(base, 3)
    counts = jax.random.randint(key_count, (DEVICES,), max(1, PMAX // 4), PMAX + 1)
    counts = counts.at[0].set(PMAX).at[STRIDE].set(PMAX)
    west_flip = jax.random.randint(key_west, (DEVICES, PMAX), 0, 2)
    north_flip = jax.random.randint(key_north, (DEVICES, PMAX), 0, 2)
    return (counts.astype(jnp.int32), west_flip.astype(jnp.int32), north_flip.astype(jnp.int32))


def draw_patch_count(key, part):
    return patch_layout(key)[0]


def link_entry(linked, device_col, slot_col, side_value, flip_col):
    shape = (DEVICES, PMAX)
    linked = jnp.broadcast_to(linked, shape)
    device_col = jnp.broadcast_to(device_col, shape)
    slot_col = jnp.broadcast_to(slot_col, shape)
    flip_col = jnp.broadcast_to(flip_col, shape)
    return jnp.stack([jnp.where(linked, device_col, -1), jnp.where(linked, slot_col * 4 + side_value, 0), jnp.where(linked, flip_col, 0)], axis=-1)


def draw_connectivity(key, part):
    counts, west_flip, north_flip = patch_layout(key)
    device_ids = jnp.arange(DEVICES, dtype=jnp.int32)[:, None]
    slot_ids = jnp.arange(PMAX, dtype=jnp.int32)[None, :]
    held = counts[:, None]
    live = slot_ids < held
    before = (device_ids - 1) % DEVICES
    after = (device_ids + 1) % DEVICES
    above = (device_ids + STRIDE) % DEVICES
    below = (device_ids - STRIDE) % DEVICES
    first = slot_ids == 0
    last = slot_ids == held - 1
    west_dev = jnp.where(first, before, device_ids)
    west_slot = jnp.where(first, counts[before] - 1, slot_ids - 1)
    east_dev = jnp.where(last, after, device_ids)
    east_slot = jnp.where(last, 0, slot_ids + 1)
    next_index = jnp.broadcast_to(jnp.minimum(slot_ids + 1, PMAX - 1), (DEVICES, PMAX))
    inner_flip = jnp.take_along_axis(west_flip, next_index, axis=1)
    east_flip = jnp.where(last, west_flip[after[:, 0], 0][:, None], inner_flip)
    south_linked = live & (slot_ids < counts[below])
    north_linked = live & (slot_ids < counts[above])
    south_flip = north_flip[below[:, 0]]
    table = jnp.stack([link_entry(live, west_dev, west_slot, 1, west_flip), link_entry(live, east_dev, east_slot, 0, east_flip), link_entry(south_linked, below, slot_ids, 3, south_flip), link_entry(north_linked, above, slot_ids, 2, north_flip)], axis=2)
    return table.reshape(DEVICES * PMAX * 4, 3).astype(jnp.int32)


def draw_moduli(key, part):
    counts = patch_layout(key)[0]
    live_slots = (jnp.arange(PMAX, dtype=jnp.int32)[None, :] < counts[:, None]).reshape(SLOTS)
    key_patch, key_cell, key_dead = jax.random.split(jax.random.fold_in(key, 23), 3)
    top_factor = 4.0
    cell = jnp.exp(jax.random.uniform(key_cell, (2, SLOTS, N, N), jnp.float32, jnp.log(0.5), jnp.log(2.0)))
    live_factor = jnp.exp(jax.random.uniform(key_patch, (SLOTS,), jnp.float32) * jnp.log(top_factor))
    dead_factor = top_factor * jnp.exp(jax.random.uniform(key_dead, (SLOTS,), jnp.float32, jnp.log(2.0), jnp.log(4.0)))
    factor = jnp.where(live_slots, live_factor, dead_factor)
    return (factor[None, :, None, None] * cell).astype(jnp.float32)


def steps_of(rng, dims, pieces, smallest, largest):
    gain = 1.0
    for axis_at, blocks in pieces:
        draws = jax.random.uniform(jax.random.fold_in(jax.random.fold_in(rng, 6), axis_at), (blocks,), jnp.float32, smallest / len(pieces), largest / len(pieces))
        gain = gain * jnp.repeat(jnp.exp(draws), dims[axis_at] // blocks).reshape((-1,) + (1,) * (len(dims) - 1 - axis_at))
    return gain


def centred(key, dims, width, reach, cuts=(), held_as=jnp.bfloat16):
    factor_of = steps_of(key, dims, cuts, -0.22, 0.18) if cuts else 1.0
    entries = jax.random.normal(key, dims, jnp.float32) * width * factor_of
    return jnp.minimum(jnp.maximum(entries, -reach), reach).astype(held_as)


def setup_inputs(seed: int = 0) -> dict:
    keys = jax.random.split(jax.random.key(seed), 9)
    fields = centred(keys[0], (5, SLOTS, N, N), 1.0, 6.0, ((1, 32),), jnp.float32)
    density = jnp.clip(jnp.exp(math.log(3.0) - 1.0986123 * jax.random.uniform(keys[1], (SLOTS, N, N), jnp.float32) ** steps_of(keys[1], (SLOTS, N, N), ((0, 32),), -0.2, 0.2)), 1.0, 3.0)
    moduli = draw_moduli(jax.random.fold_in(keys[8], 71), 0)
    metric_diag = jnp.clip(0.7 + 0.59999996 * jax.random.uniform(keys[3], (2, SLOTS, N, N), jnp.float32) ** steps_of(keys[3], (2, SLOTS, N, N), ((1, 32),), -0.2, 0.2), 0.7, 1.3)
    metric_cross = jnp.clip(jax.random.uniform(keys[4], (2, SLOTS, N, N), jnp.float32, -0.3, 0.3) * steps_of(keys[4], (2, SLOTS, N, N), ((1, 32),), -0.4, 0.0), -0.3, 0.3)
    fc_extension = centred(keys[5], (CONT, 2 * MATCH), (2 * MATCH) ** -0.5, 2.0, (), jnp.float32)
    patch_count = draw_patch_count(jax.random.fold_in(keys[8], 71), 0)
    connectivity = draw_connectivity(jax.random.fold_in(keys[8], 71), 0)
    return dict(fields=fields, density=density, moduli=moduli, metric_diag=metric_diag, metric_cross=metric_cross, fc_extension=fc_extension, patch_count=patch_count, connectivity=connectivity)


cfl_number = 0.5
penalty_weight = 0.5

def wave_speed(density, moduli, metric_diag, metric_cross):
    stiff = moduli[0] + 2.0 * moduli[1]
    xi_norm = jnp.sqrt(metric_diag[0] * metric_diag[0] + metric_cross[0] * metric_cross[0])
    eta_norm = jnp.sqrt(metric_cross[1] * metric_cross[1] + metric_diag[1] * metric_diag[1])
    return jnp.sqrt(stiff / density) * (xi_norm + eta_norm)

def boundary_lines(state):
    stacked = jnp.stack([state[:, :, 0, :], state[:, :, -1, :], state[:, :, :, 0], state[:, :, :, -1]], axis=0)
    return jnp.transpose(stacked, (2, 0, 1, 3))

def assemble(state, along_xi, along_eta, partner_lines, side_mask, density, moduli, metric_diag, metric_cross):
    grad_x = metric_diag[0] * along_xi + metric_cross[1] * along_eta
    grad_y = metric_cross[0] * along_xi + metric_diag[1] * along_eta
    lame_first = moduli[0]
    shear = moduli[1]
    stiff = lame_first + 2.0 * shear
    rate_one = (grad_x[2] + grad_y[4]) / density
    rate_two = (grad_x[4] + grad_y[3]) / density
    rate_xx = stiff * grad_x[0] + lame_first * grad_y[1]
    rate_yy = lame_first * grad_x[0] + stiff * grad_y[1]
    rate_xy = shear * (grad_y[0] + grad_x[1])
    rate = jnp.stack([rate_one, rate_two, rate_xx, rate_yy, rate_xy], axis=0)
    points = state.shape[-1]
    jump = penalty_weight * (points - 1) * (partner_lines - boundary_lines(state)) * side_mask[:, :, None, None]
    jump = jnp.transpose(jump, (1, 2, 0, 3))
    rate = rate.at[:, :, 0, :].add(jump[0])
    rate = rate.at[:, :, points - 1, :].add(jump[1])
    rate = rate.at[:, :, :, 0].add(jump[2])
    rate = rate.at[:, :, :, points - 1].add(jump[3])
    return rate

def fc_derivative(values, extension, axis):
    moved = jnp.moveaxis(values, axis, -1)
    points = moved.shape[-1]
    match_pts = extension.shape[1] // 2
    tail = jnp.concatenate([moved[..., points - match_pts:], moved[..., :match_pts]], axis=-1)
    extra_vals = jnp.einsum('...m,cm->...c', tail, extension, precision=lax.Precision.HIGHEST)
    line = jnp.concatenate([moved, extra_vals], axis=-1)
    length = line.shape[-1]
    coeffs = jnp.fft.rfft(line, axis=-1)
    wave = 2.0 * jnp.pi * jnp.arange(length // 2 + 1, dtype=jnp.float32) * (points - 1) / length
    deriv = jnp.fft.irfft(coeffs * (1j * wave), n=length, axis=-1)[..., :points]
    return jnp.moveaxis(deriv.astype(values.dtype), -1, axis)

def reference(fields, density, moduli, metric_diag, metric_cross, fc_extension, patch_count, connectivity):
    state = fields.reshape(5, DEVICES, PMAX, N, N).transpose(1, 0, 2, 3, 4)
    dens_dev = density.reshape(DEVICES, PMAX, N, N)
    moduli_dev = moduli.reshape(2, DEVICES, PMAX, N, N).transpose(1, 0, 2, 3, 4)
    diag_dev = metric_diag.reshape(2, DEVICES, PMAX, N, N).transpose(1, 0, 2, 3, 4)
    cross_dev = metric_cross.reshape(2, DEVICES, PMAX, N, N).transpose(1, 0, 2, 3, 4)
    live = jnp.arange(PMAX, dtype=jnp.int32)[None, :] < patch_count[:, None]
    side_mask = (connectivity[:, 0] >= 0).astype(jnp.float32).reshape(DEVICES, PMAX, 4)

    def device_bound(device_data):
        speeds = wave_speed(device_data[0], device_data[1], device_data[2], device_data[3])
        return jnp.max(jnp.where(device_data[4][:, None, None], speeds, jnp.float32(0.0)))
    bound = jnp.max(lax.map(device_bound, (dens_dev, moduli_dev, diag_dev, cross_dev, live)))
    time_step = cfl_number / (bound * (N - 1))
    flat_target = (jnp.maximum(connectivity[:, 0], 0) * (PMAX * 4) + connectivity[:, 1]).astype(jnp.int32)
    flip_rows = connectivity[:, 2] == 1

    def partners(current):
        lines_all = jax.vmap(boundary_lines)(current).reshape(DEVICES * PMAX * 4, 5, N)
        picked = lines_all[flat_target]
        picked = jnp.where(flip_rows[:, None, None], picked[..., ::-1], picked)
        return picked.reshape(DEVICES, PMAX, 4, 5, N)

    def advance(current):
        near_lines = partners(current)

        def one_device(device_data):
            local = device_data[0]
            along_xi = fc_derivative(local, fc_extension, 2)
            along_eta = fc_derivative(local, fc_extension, 3)
            rate = assemble(local, along_xi, along_eta, device_data[1], device_data[2], device_data[3], device_data[4], device_data[5], device_data[6])
            return local + time_step * rate
        return lax.map(one_device, (current, near_lines, side_mask, dens_dev, moduli_dev, diag_dev, cross_dev))
    middle = advance(state)
    final = advance(middle)
    result = jnp.where(live[:, None, :, None, None], 0.5 * (state + final), jnp.float32(0.0))
    return result.transpose(1, 0, 2, 3, 4).reshape(5, SLOTS, N, N)
```

```python
import functools

import jax
import jax.numpy as jnp
import numpy as np
from jax import lax
from jax.experimental import pallas as pl
from jax.experimental.pallas import tpu as pltpu
from jax.sharding import PartitionSpec as P

MESH = pl.DeviceIdType.MESH
ROWS = 8
cfl_number = 0.5
penalty_weight = 0.5


def circulant(points, extra):
    length = points + extra
    half = (length - 1) // 2
    waves = np.arange(1, half + 1, dtype=np.float64)
    weights = waves * (2.0 * np.pi * (points - 1) / length)
    shifts = np.arange(length)
    phase = 2.0 * np.pi / length * (waves[:, None] * shifts[None, :] % length)
    kernel = -(2.0 / length) * np.sum(weights[:, None] * np.sin(phase), axis=0)
    at = (np.arange(points)[:, None] - np.arange(length)[None, :]) % length
    full = kernel[at].astype(np.float32)
    padded = -(-extra // ROWS) * ROWS
    outer = np.zeros((points, points), np.float32)
    outer[:, :extra] = full[:, points:]
    return full[:, :points], outer, padded


def split(x):
    hi = x.astype(jnp.bfloat16)
    lo = (x - hi.astype(jnp.float32)).astype(jnp.bfloat16)
    return hi, lo


def kernel(
    total, subs, group,
    conn, count, fields_hbm, density_hbm, moduli_hbm, diag_hbm, cross_hbm, ext, inner, outer,
    out_hbm,
    fld, den, mod, dia, cro, rate1, rate2, dxi, deta, left, right, ext_v, cols, trans, out_v,
    lines, outbox1, outbox2, inbox1, inbox2, mine1, mine2, gather1, gather2,
    load_sem, store_sem, send1, recv1, send2, recv2, msend1, mrecv1, msend2, mrecv2,
):
    comps, slots, n, _ = fld.shape
    sides = slots * 4
    chunks = n // ROWS
    me = lax.axis_index("patch") * subs + lax.axis_index("sub")
    far = total // 2 + 1
    offsets = (1, total - 1, far, total - far)
    quotient = total // group
    rank = lax.rem(me, group)
    base = me - rank
    block = lax.div(me, group)

    def place(flat):
        return (lax.div(flat, subs), lax.rem(flat, subs))

    loads = [pltpu.make_async_copy(fields_hbm, fld, load_sem.at[0])]
    for at, (src, dst) in enumerate(
        ((density_hbm, den), (moduli_hbm, mod), (diag_hbm, dia), (cross_hbm, cro))
    ):
        loads.append(pltpu.make_async_copy(src, dst, load_sem.at[at + 1]))
    for load in loads:
        load.start()

    barrier = pltpu.get_barrier_semaphore()
    near = [lax.rem(me + off, total) for off in offsets]
    first_peers = [base + lax.rem(rank + d, group) for d in range(1, group)]
    second_peers = [lax.rem(block + d, quotient) * group + rank for d in range(1, quotient)]
    everyone = near + first_peers + second_peers
    for peer in everyone:
        pl.semaphore_signal(barrier, inc=1, device_id=place(peer), device_id_type=MESH)

    owner = [conn[s, 0] for s in range(sides)]
    strip = [conn[s, 1] for s in range(sides)]
    flip = [conn[s, 2] for s in range(sides)]
    picks = []
    for peer in near:
        seen = jnp.int32(0)
        pick = [jnp.int32(0)] * slots
        for s in range(sides):
            hit = owner[s] == peer
            for k in range(slots):
                pick[k] = jnp.where(hit & (seen == k), s, pick[k])
            seen = seen + hit.astype(jnp.int32)
        picks.append(pick)
    box, local = [], []
    for s in range(sides):
        pos = jnp.int32(0)
        for t in range(sides):
            if t != s:
                pos = pos + ((owner[t] == owner[s]) & (strip[t] < strip[s])).astype(jnp.int32)
        pos = jnp.minimum(pos, slots - 1)
        at = pos
        for o, off in enumerate(offsets):
            at = jnp.where(owner[s] == lax.rem(me + total - off, total), o * slots + pos, at)
        box.append(at)
        local.append(owner[s] == me)

    lane = lax.broadcasted_iota(jnp.int32, (ROWS, n), 1)
    low, high = lane == 0, lane == n - 1
    edge = low | high
    pairs = [(f, p, p * 8 + f) for p in range(slots) for f in range(comps)]

    def collect(state):
        def columns(c, _):
            rows = pl.ds(pl.multiple_of(c * ROWS, ROWS), ROWS)
            acc = jnp.zeros((ROWS, n), jnp.float32)
            for f, p, m in pairs:
                turned = pltpu.roll(state[f, p, rows, :], 2 * m + 1, 1)
                acc = jnp.where((lane == 2 * m) | (lane == 2 * m + 1), turned, acc)
            cols[rows, :] = acc
            return _

        lax.fori_loop(0, chunks, columns, 0, unroll=4)
        trans[...] = jnp.transpose(cols[...])
        for p in range(slots):
            lines[p * 4 + 2] = trans[pl.ds(p * 16 + 1, 8, stride=2), :]
            lines[p * 4 + 3] = trans[pl.ds(p * 16, 8, stride=2), :]
            for f in range(comps):
                lines[p * 4, pl.ds(f, 1)] = state[f, p, pl.ds(0, 1), :]
                lines[p * 4 + 1, pl.ds(f, 1)] = state[f, p, pl.ds(n - 1, 1), :]

    def post(outbox, inbox, send, recv):
        for o in range(4):
            for k in range(slots):
                outbox[o, k] = lines[picks[o][k]]
        sent = []
        for o in range(4):
            copy = pltpu.make_async_remote_copy(
                src_ref=outbox.at[o],
                dst_ref=inbox.at[pl.ds(o * slots, slots)],
                send_sem=send.at[o],
                recv_sem=recv.at[o],
                device_id=place(near[o]),
                device_id_type=MESH,
            )
            copy.start()
            sent.append(copy)
        return sent

    def jumps(inbox):
        found = []
        for s in range(sides):
            partner = jnp.where(local[s], lines[strip[s]], inbox[box[s]])
            index = jnp.where(flip[s] == 1, n - 1 - lane, lane)
            partner = jnp.take_along_axis(partner, index, axis=1)
            scale = jnp.where(owner[s] >= 0, penalty_weight * (n - 1), 0.0)
            found.append(scale * (partner - lines[s]))
        return found

    def spread(jump):
        for p in range(slots):
            trans[pl.ds(p * 16 + 1, 8, stride=2), :] = jump[p * 4 + 2]
            trans[pl.ds(p * 16, 8, stride=2), :] = jump[p * 4 + 3]
        cols[...] = jnp.transpose(trans[...])

    def derive(state):
        for f in range(comps):
            h0, l0 = split(state[f, 0])
            h1, l1 = split(state[f, 1])
            rows = jnp.concatenate(
                [jnp.concatenate([h0, l0], axis=1), jnp.concatenate([h1, l1], axis=1)], axis=0
            )
            eta = jnp.dot(rows, right[...], preferred_element_type=jnp.float32)
            both = eta[:, :n] + eta[:, n:]
            deta[f, 0] = both[:n]
            deta[f, 1] = both[n:]
            body = jnp.concatenate(
                [jnp.concatenate([h0, h1], axis=1), jnp.concatenate([l0, l1], axis=1)], axis=0
            )
            xi = jnp.dot(left[...], body, preferred_element_type=jnp.float32)
            both = xi[:n] + xi[n:]
            dxi[f, 0] = both[:, :n]
            dxi[f, 1] = both[:, n:]

    def interior(rate):
        for p in range(slots):

            def body(c, _):
                rows = pl.ds(pl.multiple_of(c * ROWS, ROWS), ROWS)
                xx, yy = dia[0, p, rows, :], dia[1, p, rows, :]
                xy, ex = cro[0, p, rows, :], cro[1, p, rows, :]
                lame, shear = mod[0, p, rows, :], mod[1, p, rows, :]
                inv = den[p, rows, :]
                stiff = lame + 2.0 * shear
                ax = [dxi[f, p, rows, :] for f in range(comps)]
                ay = [deta[f, p, rows, :] for f in range(comps)]
                gx = [xx * a + ex * b for a, b in zip(ax, ay)]
                gy = [xy * a + yy * b for a, b in zip(ax, ay)]
                rate[0, p, rows, :] = (gx[2] + gy[4]) * inv
                rate[1, p, rows, :] = (gx[4] + gy[3]) * inv
                rate[2, p, rows, :] = stiff * gx[0] + lame * gy[1]
                rate[3, p, rows, :] = lame * gx[0] + stiff * gy[1]
                rate[4, p, rows, :] = shear * (gy[0] + gx[1])
                return _

            lax.fori_loop(0, chunks, body, 0, unroll=4)

    def add_rows(rate, jump):
        for p in range(slots):
            for f in range(comps):
                for side, at in ((0, 0), (1, n - 1)):
                    spot = pl.ds(at, 1)
                    rate[f, p, spot, :] = rate[f, p, spot, :] + jump[p * 4 + side][f : f + 1]

    lines[...] = jnp.zeros_like(lines)
    trans[...] = jnp.zeros_like(trans)
    ext_v[...] = jnp.zeros_like(ext_v)
    extra, twice = ext.shape
    ext_v[pl.ds(0, extra), pl.ds(0, twice)] = ext[...]
    turned = pltpu.roll(ext_v[...], n - twice // 2, 1)
    matrix = inner[...] + jnp.dot(
        outer[...], turned, precision=lax.Precision.HIGHEST, preferred_element_type=jnp.float32
    )
    hi, lo = split(matrix)
    none = jnp.zeros_like(hi)
    left[...] = jnp.concatenate(
        [jnp.concatenate([hi, hi], axis=1), jnp.concatenate([lo, none], axis=1)], axis=0
    )
    hi, lo = split(jnp.transpose(matrix))
    right[...] = jnp.concatenate(
        [jnp.concatenate([hi, lo], axis=1), jnp.concatenate([hi, none], axis=1)], axis=0
    )

    loads[0].wait()
    collect(fld)
    pl.semaphore_wait(barrier, len(everyone))
    sent1 = post(outbox1, inbox1, send1, recv1)
    derive(fld)

    for load in loads[1:]:
        load.wait()
    top = jnp.zeros((ROWS, n), jnp.float32)
    for p in range(slots):

        def speeds(c, top):
            rows = pl.ds(pl.multiple_of(c * ROWS, ROWS), ROWS)
            xx, yy = dia[0, p, rows, :], dia[1, p, rows, :]
            xy, ex = cro[0, p, rows, :], cro[1, p, rows, :]
            stiff = mod[0, p, rows, :] + 2.0 * mod[1, p, rows, :]
            inv = 1.0 / den[p, rows, :]
            den[p, rows, :] = inv
            speed = jnp.sqrt(stiff * inv) * (
                jnp.sqrt(xx * xx + xy * xy) + jnp.sqrt(ex * ex + yy * yy)
            )
            return jnp.maximum(top, speed)

        part = lax.fori_loop(
            0, chunks, speeds, jnp.zeros((ROWS, n), jnp.float32), unroll=4
        )
        top = jnp.maximum(top, jnp.where(count[0] > p, part, 0.0))

    def share(mine, gather, peers, send, recv):
        sent = []
        for d, peer in enumerate(peers):
            copy = pltpu.make_async_remote_copy(
                src_ref=mine,
                dst_ref=gather.at[d],
                send_sem=send.at[d],
                recv_sem=recv.at[d],
                device_id=place(peer),
                device_id_type=MESH,
            )
            copy.start()
            sent.append(copy)
        return sent

    mine1[...] = jnp.max(top, axis=0, keepdims=True)
    shared1 = share(mine1, gather1, first_peers, msend1, mrecv1)
    interior(rate1)

    for copy in sent1:
        copy.wait_recv()
    jump1 = jumps(inbox1)
    collect(rate1)
    for p in range(slots):
        west, east, south, north = jump1[p * 4 : p * 4 + 4]
        lines[p * 4] += (
            west + jnp.where(low, south, 0.0) + jnp.where(high, pltpu.roll(north, n - 1, 1), 0.0)
        )
        lines[p * 4 + 1] += (
            east + jnp.where(low, pltpu.roll(south, 1, 1), 0.0) + jnp.where(high, north, 0.0)
        )
        lines[p * 4 + 2] += (
            south + jnp.where(low, west, 0.0) + jnp.where(high, pltpu.roll(east, n - 1, 1), 0.0)
        )
        lines[p * 4 + 3] += (
            north + jnp.where(low, pltpu.roll(west, 1, 1), 0.0) + jnp.where(high, east, 0.0)
        )
    sent2 = post(outbox2, inbox2, send2, recv2)

    for copy in shared1:
        copy.wait_recv()
    best = mine1[...]
    for d in range(len(first_peers)):
        best = jnp.maximum(best, gather1[d])
    mine2[...] = best
    shared2 = share(mine2, gather2, second_peers, msend2, mrecv2)

    spread(jump1)
    add_rows(rate1, jump1)

    def patch_up(c, _):
        rows = pl.ds(pl.multiple_of(c * ROWS, ROWS), ROWS)
        both = cols[rows, :]
        for f, p, m in pairs:
            side = pltpu.roll(both, n - (2 * m + 1), 1)
            rate1[f, p, rows, :] = rate1[f, p, rows, :] + jnp.where(edge, side, 0.0)
        return _

    lax.fori_loop(0, chunks, patch_up, 0, unroll=4)
    derive(rate1)
    interior(rate2)

    for copy in shared2:
        copy.wait_recv()
    for d in range(len(second_peers)):
        best = jnp.maximum(best, gather2[d])
    bound = jnp.max(best, axis=1, keepdims=True)
    step = jnp.broadcast_to(cfl_number / (bound * (n - 1)), (ROWS, n))
    half = 0.5 * step * step

    for copy in sent2:
        copy.wait_recv()
    jump2 = jumps(inbox2)
    spread(jump2)
    add_rows(rate2, jump2)
    stores = []
    for p in range(slots):
        live = count[0] > p

        def finish(c, _):
            rows = pl.ds(pl.multiple_of(c * ROWS, ROWS), ROWS)
            both = cols[rows, :]
            for f in range(comps):
                side = pltpu.roll(both, n - (2 * (p * 8 + f) + 1), 1)
                second = rate2[f, p, rows, :] + jnp.where(edge, side, 0.0)
                value = fld[f, p, rows, :] + step * rate1[f, p, rows, :] + half * second
                out_v[f, p, rows, :] = jnp.where(live, value, 0.0)
            return _

        lax.fori_loop(0, chunks, finish, 0, unroll=4)
        store = pltpu.make_async_copy(out_v.at[:, p], out_hbm.at[:, p], store_sem.at[p])
        store.start()
        stores.append(store)
    for copy in sent1 + sent2 + shared1 + shared2:
        copy.wait_send()
    for store in stores:
        store.wait()


def shards(
    total, subs, fields, density, moduli, metric_diag, metric_cross, extension, count, connectivity
):
    comps, slots, n, _ = fields.shape
    group = max(g for g in range(1, total) if total % g == 0 and g * g <= total)
    inner, outer, _ = circulant(n, extension.shape[0])
    f32 = jnp.float32
    vmem = pl.BlockSpec(memory_space=pltpu.VMEM)
    smem = pl.BlockSpec(memory_space=pltpu.SMEM)
    hbm = pl.BlockSpec(memory_space=pl.ANY)
    state = pltpu.VMEM(fields.shape, f32)
    dma = pltpu.SemaphoreType.DMA
    boxed = pltpu.VMEM((4, slots, 8, n), f32)
    arrived = pltpu.VMEM((4 * slots, 8, n), f32)
    quotient = total // group
    return pl.pallas_call(
        functools.partial(kernel, total, subs, group),
        out_shape=jax.ShapeDtypeStruct(fields.shape, f32),
        in_specs=[smem, smem] + [hbm] * 5 + [vmem] * 3,
        out_specs=hbm,
        scratch_shapes=[
            state,
            pltpu.VMEM(density.shape, f32),
            pltpu.VMEM(moduli.shape, f32),
            pltpu.VMEM(metric_diag.shape, f32),
            pltpu.VMEM(metric_cross.shape, f32),
            state, state, state, state,
            pltpu.VMEM((2 * n, 2 * n), jnp.bfloat16),
            pltpu.VMEM((2 * n, 2 * n), jnp.bfloat16),
            pltpu.VMEM((n, n), f32),
            pltpu.VMEM((n, n), f32),
            pltpu.VMEM((n, n), f32),
            state,
            pltpu.VMEM((slots * 4, 8, n), f32),
            boxed, boxed, arrived, arrived,
            pltpu.VMEM((1, n), f32),
            pltpu.VMEM((1, n), f32),
            pltpu.VMEM((group - 1, 1, n), f32),
            pltpu.VMEM((quotient - 1, 1, n), f32),
            dma((5,)), dma((slots,)),
            dma((4,)), dma((4,)), dma((4,)), dma((4,)),
            dma((group - 1,)), dma((group - 1,)), dma((quotient - 1,)), dma((quotient - 1,)),
        ],
        compiler_params=pltpu.CompilerParams(collective_id=0, has_side_effects=True),
    )(connectivity, count, fields, density, moduli, metric_diag, metric_cross, extension,
      jnp.asarray(inner), jnp.asarray(outer))


def solution(mesh):
    placed = (
        P(None, ("patch", "sub"), None, None),
        P(("patch", "sub"), None, None),
        P(None, ("patch", "sub"), None, None),
        P(None, ("patch", "sub"), None, None),
        P(None, ("patch", "sub"), None, None),
        P(),
        P(("patch", "sub")),
        P(("patch", "sub"), None),
    )
    total = mesh.shape["patch"] * mesh.shape["sub"]
    return jax.shard_map(
        functools.partial(shards, total, mesh.shape["sub"]),
        mesh=mesh,
        in_specs=placed,
        out_specs=P(None, ("patch", "sub"), None, None),
        check_vma=False,
    )
```

```python
import functools

import jax
import jax.numpy as jnp
import numpy as np
from jax import lax
from jax.experimental import pallas as pl
from jax.experimental.pallas import tpu as pltpu
from jax.sharding import PartitionSpec as P

MESH = pl.DeviceIdType.MESH
ROWS = 8
cfl_number = 0.5
penalty_weight = 0.5


def circulant(points, extra):
    length = points + extra
    half = (length - 1) // 2
    waves = np.arange(1, half + 1, dtype=np.float64)
    weights = waves * (2.0 * np.pi * (points - 1) / length)
    shifts = np.arange(length)
    phase = 2.0 * np.pi / length * (waves[:, None] * shifts[None, :] % length)
    kernel = -(2.0 / length) * np.sum(weights[:, None] * np.sin(phase), axis=0)
    at = (np.arange(points)[:, None] - np.arange(length)[None, :]) % length
    full = kernel[at].astype(np.float32)
    padded = -(-extra // ROWS) * ROWS
    outer = np.zeros((points, points), np.float32)
    outer[:, :extra] = full[:, points:]
    return full[:, :points], outer, padded


def split(x):
    hi = x.astype(jnp.bfloat16)
    lo = (x - hi.astype(jnp.float32)).astype(jnp.bfloat16)
    return hi, lo


def kernel(
    total, subs, group,
    conn, count, fields_hbm, density_hbm, moduli_hbm, diag_hbm, cross_hbm, ext, inner, outer,
    out_v,
    fld, den, mod, dia, cro, rate1, rate2, dxi, deta, left, right, ext_v, cols, trans,
    lines, lines2, outbox1, outbox2, inbox1, inbox2, mine1, mine2, gather1, gather2,
    load_sem, send1, recv1, send2, recv2, msend1, mrecv1, msend2, mrecv2,
):
    comps, slots, n, _ = fld.shape
    sides = slots * 4
    chunks = n // ROWS
    me = lax.axis_index("patch") * subs + lax.axis_index("sub")
    far = total // 2 + 1
    offsets = (1, total - 1, far, total - far)
    quotient = total // group
    rank = lax.rem(me, group)
    base = me - rank
    block = lax.div(me, group)

    def place(flat):
        return (lax.div(flat, subs), lax.rem(flat, subs))

    loads = [pltpu.make_async_copy(fields_hbm, fld, load_sem.at[0])]
    for at, (src, dst) in enumerate(
        ((density_hbm, den), (moduli_hbm, mod), (diag_hbm, dia), (cross_hbm, cro))
    ):
        loads.append(pltpu.make_async_copy(src, dst, load_sem.at[at + 1]))
    for load in loads:
        load.start()

    barrier = pltpu.get_barrier_semaphore()
    near = [lax.rem(me + off, total) for off in offsets]
    first_peers = [base + lax.rem(rank + d, group) for d in range(1, group)]
    second_peers = [lax.rem(block + d, quotient) * group + rank for d in range(1, quotient)]
    everyone = near + first_peers + second_peers
    for peer in everyone:
        pl.semaphore_signal(barrier, inc=1, device_id=place(peer), device_id_type=MESH)

    owner = [conn[0, s] for s in range(sides)]
    strip = [conn[1, s] for s in range(sides)]
    flip = [conn[2, s] for s in range(sides)]
    picks = []
    for peer in near:
        seen = jnp.int32(0)
        pick = [jnp.int32(0)] * slots
        for s in range(sides):
            hit = owner[s] == peer
            for k in range(slots):
                pick[k] = jnp.where(hit & (seen == k), s, pick[k])
            seen = seen + hit.astype(jnp.int32)
        picks.append(pick)
    box, local = [], []
    for s in range(sides):
        pos = jnp.int32(0)
        for t in range(sides):
            if t != s:
                pos = pos + ((owner[t] == owner[s]) & (strip[t] < strip[s])).astype(jnp.int32)
        pos = jnp.minimum(pos, slots - 1)
        at = pos
        for o, off in enumerate(offsets):
            at = jnp.where(owner[s] == lax.rem(me + total - off, total), o * slots + pos, at)
        box.append(at)
        local.append(owner[s] == me)

    lane = lax.broadcasted_iota(jnp.int32, (ROWS, n), 1)
    low, high = lane == 0, lane == n - 1
    edge = low | high
    pairs = [(f, p, p * 8 + f) for p in range(slots) for f in range(comps)]

    def collect(state, lines):
        def columns(c, _):
            rows = pl.ds(pl.multiple_of(c * ROWS, ROWS), ROWS)
            acc = jnp.zeros((ROWS, n), jnp.float32)
            for f, p, m in pairs:
                turned = pltpu.roll(state[f, p, rows, :], 2 * m + 1, 1)
                acc = jnp.where((lane == 2 * m) | (lane == 2 * m + 1), turned, acc)
            cols[rows, :] = acc
            return _

        lax.fori_loop(0, chunks, columns, 0, unroll=4)
        trans[...] = jnp.transpose(cols[...])
        for p in range(slots):
            lines[p * 4 + 2] = trans[pl.ds(p * 16 + 1, 8, stride=2), :]
            lines[p * 4 + 3] = trans[pl.ds(p * 16, 8, stride=2), :]
            for f in range(comps):
                lines[p * 4, pl.ds(f, 1)] = state[f, p, pl.ds(0, 1), :]
                lines[p * 4 + 1, pl.ds(f, 1)] = state[f, p, pl.ds(n - 1, 1), :]

    def post(lines, outbox, inbox, send, recv):
        for o in range(4):
            for k in range(slots):
                outbox[o, k] = lines[picks[o][k]]
        sent = []
        for o in range(4):
            copy = pltpu.make_async_remote_copy(
                src_ref=outbox.at[o],
                dst_ref=inbox.at[pl.ds(o * slots, slots)],
                send_sem=send.at[o],
                recv_sem=recv.at[o],
                device_id=place(near[o]),
                device_id_type=MESH,
            )
            copy.start()
            sent.append(copy)
        return sent

    def jumps(lines, inbox):
        found = []
        for s in range(sides):
            partner = jnp.where(local[s], lines[strip[s]], inbox[box[s]])
            index = jnp.where(flip[s] == 1, n - 1 - lane, lane)
            partner = jnp.take_along_axis(partner, index, axis=1)
            scale = jnp.where(owner[s] >= 0, penalty_weight * (n - 1), 0.0)
            found.append(scale * (partner - lines[s]))
        return found

    def spread(jump):
        for p in range(slots):
            trans[pl.ds(p * 16 + 1, 8, stride=2), :] = jump[p * 4 + 2]
            trans[pl.ds(p * 16, 8, stride=2), :] = jump[p * 4 + 3]
        cols[...] = jnp.transpose(trans[...])

    def derive(state):
        for f in range(comps):
            h0, l0 = split(state[f, 0])
            h1, l1 = split(state[f, 1])
            rows = jnp.concatenate(
                [jnp.concatenate([h0, l0], axis=1), jnp.concatenate([h1, l1], axis=1)], axis=0
            )
            eta = jnp.dot(rows, right[...], preferred_element_type=jnp.float32)
            both = eta[:, :n] + eta[:, n:]
            deta[f, 0] = both[:n]
            deta[f, 1] = both[n:]
            body = jnp.concatenate(
                [jnp.concatenate([h0, h1], axis=1), jnp.concatenate([l0, l1], axis=1)], axis=0
            )
            xi = jnp.dot(left[...], body, preferred_element_type=jnp.float32)
            both = xi[:n] + xi[n:]
            dxi[f, 0] = both[:, :n]
            dxi[f, 1] = both[:, n:]

    def interior(rate):
        for p in range(slots):

            def body(c, _):
                rows = pl.ds(pl.multiple_of(c * ROWS, ROWS), ROWS)
                xx, yy = dia[0, p, rows, :], dia[1, p, rows, :]
                xy, ex = cro[0, p, rows, :], cro[1, p, rows, :]
                lame, shear = mod[0, p, rows, :], mod[1, p, rows, :]
                inv = den[p, rows, :]
                stiff = lame + 2.0 * shear
                ax = [dxi[f, p, rows, :] for f in range(comps)]
                ay = [deta[f, p, rows, :] for f in range(comps)]
                gx = [xx * a + ex * b for a, b in zip(ax, ay)]
                gy = [xy * a + yy * b for a, b in zip(ax, ay)]
                rate[0, p, rows, :] = (gx[2] + gy[4]) * inv
                rate[1, p, rows, :] = (gx[4] + gy[3]) * inv
                rate[2, p, rows, :] = stiff * gx[0] + lame * gy[1]
                rate[3, p, rows, :] = lame * gx[0] + stiff * gy[1]
                rate[4, p, rows, :] = shear * (gy[0] + gx[1])
                return _

            lax.fori_loop(0, chunks, body, 0, unroll=4)

    def add_rows(rate, jump):
        for p in range(slots):
            for f in range(comps):
                for side, at in ((0, 0), (1, n - 1)):
                    spot = pl.ds(at, 1)
                    rate[f, p, spot, :] = rate[f, p, spot, :] + jump[p * 4 + side][f : f + 1]

    lines[...] = jnp.zeros_like(lines)
    lines2[...] = jnp.zeros_like(lines2)
    trans[...] = jnp.zeros_like(trans)
    ext_v[...] = jnp.zeros_like(ext_v)
    twice, extra = ext.shape
    ext_v[pl.ds(0, twice), pl.ds(0, extra)] = ext[...]
    turned = pltpu.roll(ext_v[...], n - twice // 2, 0)
    matrix = inner[...] + lax.dot_general(
        outer[...],
        turned,
        (((1,), (1,)), ((), ())),
        precision=lax.Precision.HIGHEST,
        preferred_element_type=jnp.float32,
    )
    hi, lo = split(matrix)
    none = jnp.zeros_like(hi)
    left[...] = jnp.concatenate(
        [jnp.concatenate([hi, hi], axis=1), jnp.concatenate([lo, none], axis=1)], axis=0
    )
    hi, lo = split(jnp.transpose(matrix))
    right[...] = jnp.concatenate(
        [jnp.concatenate([hi, lo], axis=1), jnp.concatenate([hi, none], axis=1)], axis=0
    )

    loads[0].wait()
    collect(fld, lines)
    pl.semaphore_wait(barrier, len(everyone))
    sent1 = post(lines, outbox1, inbox1, send1, recv1)
    derive(fld)

    for load in loads[1:]:
        load.wait()
    top = jnp.zeros((ROWS, n), jnp.float32)
    for p in range(slots):

        def speeds(c, top):
            rows = pl.ds(pl.multiple_of(c * ROWS, ROWS), ROWS)
            xx, yy = dia[0, p, rows, :], dia[1, p, rows, :]
            xy, ex = cro[0, p, rows, :], cro[1, p, rows, :]
            stiff = mod[0, p, rows, :] + 2.0 * mod[1, p, rows, :]
            inv = 1.0 / den[p, rows, :]
            den[p, rows, :] = inv
            speed = jnp.sqrt(stiff * inv) * (
                jnp.sqrt(xx * xx + xy * xy) + jnp.sqrt(ex * ex + yy * yy)
            )
            return jnp.maximum(top, speed)

        part = lax.fori_loop(
            0, chunks, speeds, jnp.zeros((ROWS, n), jnp.float32), unroll=4
        )
        top = jnp.maximum(top, jnp.where(count[0] > p, part, 0.0))

    def share(mine, gather, peers, send, recv):
        sent = []
        for d, peer in enumerate(peers):
            copy = pltpu.make_async_remote_copy(
                src_ref=mine,
                dst_ref=gather.at[d],
                send_sem=send.at[d],
                recv_sem=recv.at[d],
                device_id=place(peer),
                device_id_type=MESH,
            )
            copy.start()
            sent.append(copy)
        return sent

    mine1[...] = jnp.max(top, axis=0, keepdims=True)
    shared1 = share(mine1, gather1, first_peers, msend1, mrecv1)
    interior(rate1)

    collect(rate1, lines2)
    for copy in sent1:
        copy.wait_recv()
    jump1 = jumps(lines, inbox1)
    for p in range(slots):
        west, east, south, north = jump1[p * 4 : p * 4 + 4]
        lines2[p * 4] += (
            west + jnp.where(low, south, 0.0) + jnp.where(high, pltpu.roll(north, n - 1, 1), 0.0)
        )
        lines2[p * 4 + 1] += (
            east + jnp.where(low, pltpu.roll(south, 1, 1), 0.0) + jnp.where(high, north, 0.0)
        )
        lines2[p * 4 + 2] += (
            south + jnp.where(low, west, 0.0) + jnp.where(high, pltpu.roll(east, n - 1, 1), 0.0)
        )
        lines2[p * 4 + 3] += (
            north + jnp.where(low, pltpu.roll(west, 1, 1), 0.0) + jnp.where(high, east, 0.0)
        )
    sent2 = post(lines2, outbox2, inbox2, send2, recv2)

    for copy in shared1:
        copy.wait_recv()
    best = mine1[...]
    for d in range(len(first_peers)):
        best = jnp.maximum(best, gather1[d])
    mine2[...] = best
    shared2 = share(mine2, gather2, second_peers, msend2, mrecv2)

    spread(jump1)
    add_rows(rate1, jump1)

    def patch_up(c, _):
        rows = pl.ds(pl.multiple_of(c * ROWS, ROWS), ROWS)
        both = cols[rows, :]
        for f, p, m in pairs:
            side = pltpu.roll(both, n - (2 * m + 1), 1)
            rate1[f, p, rows, :] = rate1[f, p, rows, :] + jnp.where(edge, side, 0.0)
        return _

    lax.fori_loop(0, chunks, patch_up, 0, unroll=4)
    derive(rate1)
    interior(rate2)

    for copy in shared2:
        copy.wait_recv()
    for d in range(len(second_peers)):
        best = jnp.maximum(best, gather2[d])
    bound = jnp.max(best, axis=1, keepdims=True)
    step = jnp.broadcast_to(cfl_number / (bound * (n - 1)), (ROWS, n))
    half = 0.5 * step * step

    for copy in sent2:
        copy.wait_recv()
    jump2 = jumps(lines2, inbox2)
    spread(jump2)
    add_rows(rate2, jump2)
    for p in range(slots):
        live = count[0] > p

        def finish(c, _):
            rows = pl.ds(pl.multiple_of(c * ROWS, ROWS), ROWS)
            both = cols[rows, :]
            for f in range(comps):
                side = pltpu.roll(both, n - (2 * (p * 8 + f) + 1), 1)
                second = rate2[f, p, rows, :] + jnp.where(edge, side, 0.0)
                value = fld[f, p, rows, :] + step * rate1[f, p, rows, :] + half * second
                out_v[f, p, rows, :] = jnp.where(live, value, 0.0)
            return _

        lax.fori_loop(0, chunks, finish, 0, unroll=4)
    for copy in sent1 + sent2 + shared1 + shared2:
        copy.wait_send()


def shards(
    total, subs, fields, density, moduli, metric_diag, metric_cross, extension, count, connectivity
):
    comps, slots, n, _ = fields.shape
    group = max(g for g in range(1, total) if total % g == 0 and g * g <= total)
    inner, outer, _ = circulant(n, extension.shape[0])
    f32 = jnp.float32
    vmem = pl.BlockSpec(memory_space=pltpu.VMEM)
    smem = pl.BlockSpec(memory_space=pltpu.SMEM)
    hbm = pl.BlockSpec(memory_space=pltpu.HBM)
    state = pltpu.VMEM(fields.shape, f32)
    dma = pltpu.SemaphoreType.DMA
    boxed = pltpu.VMEM((4, slots, 8, n), f32)
    arrived = pltpu.VMEM((4 * slots, 8, n), f32)
    quotient = total // group
    return pl.pallas_call(
        functools.partial(kernel, total, subs, group),
        out_shape=pltpu.VMEM(fields.shape, f32),
        in_specs=[smem, smem] + [hbm] * 5 + [vmem] * 3,
        out_specs=vmem,
        scratch_shapes=[
            state,
            pltpu.VMEM(density.shape, f32),
            pltpu.VMEM(moduli.shape, f32),
            pltpu.VMEM(metric_diag.shape, f32),
            pltpu.VMEM(metric_cross.shape, f32),
            state, state, state, state,
            pltpu.VMEM((2 * n, 2 * n), jnp.bfloat16),
            pltpu.VMEM((2 * n, 2 * n), jnp.bfloat16),
            pltpu.VMEM((n, n), f32),
            pltpu.VMEM((n, n), f32),
            pltpu.VMEM((n, n), f32),
            pltpu.VMEM((slots * 4, 8, n), f32),
            pltpu.VMEM((slots * 4, 8, n), f32),
            boxed, boxed, arrived, arrived,
            pltpu.VMEM((1, n), f32),
            pltpu.VMEM((1, n), f32),
            pltpu.VMEM((group - 1, 1, n), f32),
            pltpu.VMEM((quotient - 1, 1, n), f32),
            dma((5,)),
            dma((4,)), dma((4,)), dma((4,)), dma((4,)),
            dma((group - 1,)), dma((group - 1,)), dma((quotient - 1,)), dma((quotient - 1,)),
        ],
        compiler_params=pltpu.CompilerParams(collective_id=0, has_side_effects=True),
    )(connectivity.T, count, fields, density, moduli, metric_diag, metric_cross, extension.T,
      jnp.asarray(inner), jnp.asarray(outer))


def solution(mesh):
    placed = (
        P(None, ("patch", "sub"), None, None),
        P(("patch", "sub"), None, None),
        P(None, ("patch", "sub"), None, None),
        P(None, ("patch", "sub"), None, None),
        P(None, ("patch", "sub"), None, None),
        P(),
        P(("patch", "sub")),
        P(("patch", "sub"), None),
    )
    total = mesh.shape["patch"] * mesh.shape["sub"]
    return jax.shard_map(
        functools.partial(shards, total, mesh.shape["sub"]),
        mesh=mesh,
        in_specs=placed,
        out_specs=P(None, ("patch", "sub"), None, None),
        check_vma=False,
    )
```

```python
import functools

import jax
import jax.numpy as jnp
import numpy as np
from jax import lax
from jax.experimental import pallas as pl
from jax.experimental.pallas import tpu as pltpu
from jax.sharding import PartitionSpec as P

MESH = pl.DeviceIdType.MESH
ROWS = 8
cfl_number = 0.5
penalty_weight = 0.5


def circulant(points, extra):
    length = points + extra
    half = (length - 1) // 2
    waves = np.arange(1, half + 1, dtype=np.float64)
    weights = waves * (2.0 * np.pi * (points - 1) / length)
    shifts = np.arange(length)
    phase = 2.0 * np.pi / length * (waves[:, None] * shifts[None, :] % length)
    kernel = -(2.0 / length) * np.sum(weights[:, None] * np.sin(phase), axis=0)
    at = (np.arange(points)[:, None] - np.arange(length)[None, :]) % length
    full = kernel[at].astype(np.float32)
    padded = -(-extra // ROWS) * ROWS
    outer = np.zeros((points, points), np.float32)
    outer[:, :extra] = full[:, points:]
    return full[:, :points], outer, padded


def split(x):
    hi = x.astype(jnp.bfloat16)
    lo = (x - hi.astype(jnp.float32)).astype(jnp.bfloat16)
    return hi, lo


def kernel(
    total, subs, group,
    conn, count, fields_hbm, density_hbm, moduli_hbm, diag_hbm, cross_hbm, ext, inner, outer,
    out_v,
    fld, den, mod, dia, cro, rate1, rate2, dxi, deta, left, right, ext_v, cols, trans,
    lines, lines2, outbox1, outbox2, inbox1, inbox2, mine1, mine2, gather1, gather2,
    load_sem, send1, recv1, send2, recv2, msend1, mrecv1, msend2, mrecv2,
):
    comps, slots, n, _ = fld.shape
    sides = slots * 4
    chunks = n // ROWS
    me = lax.axis_index("patch") * subs + lax.axis_index("sub")
    far = total // 2 + 1
    offsets = (1, total - 1, far, total - far)
    quotient = total // group
    rank = lax.rem(me, group)
    base = me - rank
    block = lax.div(me, group)

    def place(flat):
        return (lax.div(flat, subs), lax.rem(flat, subs))

    loads = [pltpu.make_async_copy(fields_hbm, fld, load_sem.at[0])]
    for at, (src, dst) in enumerate(
        ((density_hbm, den), (moduli_hbm, mod), (diag_hbm, dia), (cross_hbm, cro))
    ):
        loads.append(pltpu.make_async_copy(src, dst, load_sem.at[at + 1]))
    for load in loads:
        load.start()

    barrier = pltpu.get_barrier_semaphore()
    near = [lax.rem(me + off, total) for off in offsets]
    first_peers = [base + lax.rem(rank + d, group) for d in range(1, group)]
    second_peers = [lax.rem(block + d, quotient) * group + rank for d in range(1, quotient)]
    everyone = near + first_peers + second_peers
    for peer in everyone:
        pl.semaphore_signal(barrier, inc=1, device_id=place(peer), device_id_type=MESH)

    owner = [conn[0, s] for s in range(sides)]
    strip = [conn[1, s] for s in range(sides)]
    flip = [conn[2, s] for s in range(sides)]
    picks = []
    for peer in near:
        seen = jnp.int32(0)
        pick = [jnp.int32(0)] * slots
        for s in range(sides):
            hit = owner[s] == peer
            for k in range(slots):
                pick[k] = jnp.where(hit & (seen == k), s, pick[k])
            seen = seen + hit.astype(jnp.int32)
        picks.append(pick)
    box, local = [], []
    for s in range(sides):
        pos = jnp.int32(0)
        for t in range(sides):
            if t != s:
                pos = pos + ((owner[t] == owner[s]) & (strip[t] < strip[s])).astype(jnp.int32)
        pos = jnp.minimum(pos, slots - 1)
        at = pos
        for o, off in enumerate(offsets):
            at = jnp.where(owner[s] == lax.rem(me + total - off, total), o * slots + pos, at)
        box.append(at)
        local.append(owner[s] == me)

    lane = lax.broadcasted_iota(jnp.int32, (ROWS, n), 1)
    low, high = lane == 0, lane == n - 1
    edge = low | high
    pairs = [(f, p, p * 8 + f) for p in range(slots) for f in range(comps)]

    def collect(state, lines):
        def columns(c, _):
            rows = pl.ds(pl.multiple_of(c * ROWS, ROWS), ROWS)
            acc = jnp.zeros((ROWS, n), jnp.float32)
            for f, p, m in pairs:
                turned = pltpu.roll(state[f, p, rows, :], 2 * m + 1, 1)
                acc = jnp.where((lane == 2 * m) | (lane == 2 * m + 1), turned, acc)
            cols[rows, :] = acc
            return _

        lax.fori_loop(0, chunks, columns, 0, unroll=chunks)
        trans[...] = jnp.transpose(cols[...])
        for p in range(slots):
            lines[p * 4 + 2] = trans[pl.ds(p * 16 + 1, 8, stride=2), :]
            lines[p * 4 + 3] = trans[pl.ds(p * 16, 8, stride=2), :]
            for f in range(comps):
                lines[p * 4, pl.ds(f, 1)] = state[f, p, pl.ds(0, 1), :]
                lines[p * 4 + 1, pl.ds(f, 1)] = state[f, p, pl.ds(n - 1, 1), :]

    def post(lines, outbox, inbox, send, recv):
        for o in range(4):
            for k in range(slots):
                outbox[o, k] = lines[picks[o][k]]
        sent = []
        for o in range(4):
            copy = pltpu.make_async_remote_copy(
                src_ref=outbox.at[o],
                dst_ref=inbox.at[pl.ds(o * slots, slots)],
                send_sem=send.at[o],
                recv_sem=recv.at[o],
                device_id=place(near[o]),
                device_id_type=MESH,
            )
            copy.start()
            sent.append(copy)
        return sent

    def jumps(lines, inbox):
        found = []
        for s in range(sides):
            partner = jnp.where(local[s], lines[strip[s]], inbox[box[s]])
            index = jnp.where(flip[s] == 1, n - 1 - lane, lane)
            partner = jnp.take_along_axis(partner, index, axis=1)
            scale = jnp.where(owner[s] >= 0, penalty_weight * (n - 1), 0.0)
            found.append(scale * (partner - lines[s]))
        return found

    def spread(jump):
        for p in range(slots):
            trans[pl.ds(p * 16 + 1, 8, stride=2), :] = jump[p * 4 + 2]
            trans[pl.ds(p * 16, 8, stride=2), :] = jump[p * 4 + 3]
        cols[...] = jnp.transpose(trans[...])

    def derive(state):
        for f in range(comps):
            h0, l0 = split(state[f, 0])
            h1, l1 = split(state[f, 1])
            rows = jnp.concatenate(
                [jnp.concatenate([h0, l0], axis=1), jnp.concatenate([h1, l1], axis=1)], axis=0
            )
            eta = jnp.dot(rows, right[...], preferred_element_type=jnp.float32)
            both = eta[:, :n] + eta[:, n:]
            deta[f, 0] = both[:n]
            deta[f, 1] = both[n:]
            body = jnp.concatenate(
                [jnp.concatenate([h0, h1], axis=1), jnp.concatenate([l0, l1], axis=1)], axis=0
            )
            xi = jnp.dot(left[...], body, preferred_element_type=jnp.float32)
            both = xi[:n] + xi[n:]
            dxi[f, 0] = both[:, :n]
            dxi[f, 1] = both[:, n:]

    def interior(rate):
        for p in range(slots):

            def body(c, _):
                rows = pl.ds(pl.multiple_of(c * ROWS, ROWS), ROWS)
                xx, yy = dia[0, p, rows, :], dia[1, p, rows, :]
                xy, ex = cro[0, p, rows, :], cro[1, p, rows, :]
                lame, shear = mod[0, p, rows, :], mod[1, p, rows, :]
                inv = den[p, rows, :]
                stiff = lame + 2.0 * shear
                ax = [dxi[f, p, rows, :] for f in range(comps)]
                ay = [deta[f, p, rows, :] for f in range(comps)]
                gx = [xx * a + ex * b for a, b in zip(ax, ay)]
                gy = [xy * a + yy * b for a, b in zip(ax, ay)]
                rate[0, p, rows, :] = (gx[2] + gy[4]) * inv
                rate[1, p, rows, :] = (gx[4] + gy[3]) * inv
                rate[2, p, rows, :] = stiff * gx[0] + lame * gy[1]
                rate[3, p, rows, :] = lame * gx[0] + stiff * gy[1]
                rate[4, p, rows, :] = shear * (gy[0] + gx[1])
                return _

            lax.fori_loop(0, chunks, body, 0, unroll=chunks)

    def add_rows(rate, jump):
        for p in range(slots):
            for f in range(comps):
                for side, at in ((0, 0), (1, n - 1)):
                    spot = pl.ds(at, 1)
                    rate[f, p, spot, :] = rate[f, p, spot, :] + jump[p * 4 + side][f : f + 1]

    lines[...] = jnp.zeros_like(lines)
    lines2[...] = jnp.zeros_like(lines2)
    trans[...] = jnp.zeros_like(trans)
    ext_v[...] = jnp.zeros_like(ext_v)
    twice, extra = ext.shape
    ext_v[pl.ds(0, twice), pl.ds(0, extra)] = ext[...]
    turned = pltpu.roll(ext_v[...], n - twice // 2, 0)
    matrix = inner[...] + lax.dot_general(
        outer[...],
        turned,
        (((1,), (1,)), ((), ())),
        precision=lax.Precision.HIGHEST,
        preferred_element_type=jnp.float32,
    )
    hi, lo = split(matrix)
    none = jnp.zeros_like(hi)
    left[...] = jnp.concatenate(
        [jnp.concatenate([hi, hi], axis=1), jnp.concatenate([lo, none], axis=1)], axis=0
    )
    hi, lo = split(jnp.transpose(matrix))
    right[...] = jnp.concatenate(
        [jnp.concatenate([hi, lo], axis=1), jnp.concatenate([hi, none], axis=1)], axis=0
    )

    loads[0].wait()
    collect(fld, lines)
    pl.semaphore_wait(barrier, len(everyone))
    sent1 = post(lines, outbox1, inbox1, send1, recv1)
    derive(fld)

    for load in loads[1:]:
        load.wait()
    top = jnp.zeros((ROWS, n), jnp.float32)
    for p in range(slots):

        def speeds(c, top):
            rows = pl.ds(pl.multiple_of(c * ROWS, ROWS), ROWS)
            xx, yy = dia[0, p, rows, :], dia[1, p, rows, :]
            xy, ex = cro[0, p, rows, :], cro[1, p, rows, :]
            stiff = mod[0, p, rows, :] + 2.0 * mod[1, p, rows, :]
            inv = 1.0 / den[p, rows, :]
            den[p, rows, :] = inv
            speed = jnp.sqrt(stiff * inv) * (
                jnp.sqrt(xx * xx + xy * xy) + jnp.sqrt(ex * ex + yy * yy)
            )
            return jnp.maximum(top, speed)

        part = lax.fori_loop(
            0, chunks, speeds, jnp.zeros((ROWS, n), jnp.float32), unroll=chunks
        )
        top = jnp.maximum(top, jnp.where(count[0] > p, part, 0.0))

    def share(mine, gather, peers, send, recv):
        sent = []
        for d, peer in enumerate(peers):
            copy = pltpu.make_async_remote_copy(
                src_ref=mine,
                dst_ref=gather.at[d],
                send_sem=send.at[d],
                recv_sem=recv.at[d],
                device_id=place(peer),
                device_id_type=MESH,
            )
            copy.start()
            sent.append(copy)
        return sent

    mine1[...] = jnp.max(top, axis=0, keepdims=True)
    shared1 = share(mine1, gather1, first_peers, msend1, mrecv1)
    interior(rate1)

    collect(rate1, lines2)
    for copy in sent1:
        copy.wait_recv()
    jump1 = jumps(lines, inbox1)
    for p in range(slots):
        west, east, south, north = jump1[p * 4 : p * 4 + 4]
        lines2[p * 4] += (
            west + jnp.where(low, south, 0.0) + jnp.where(high, pltpu.roll(north, n - 1, 1), 0.0)
        )
        lines2[p * 4 + 1] += (
            east + jnp.where(low, pltpu.roll(south, 1, 1), 0.0) + jnp.where(high, north, 0.0)
        )
        lines2[p * 4 + 2] += (
            south + jnp.where(low, west, 0.0) + jnp.where(high, pltpu.roll(east, n - 1, 1), 0.0)
        )
        lines2[p * 4 + 3] += (
            north + jnp.where(low, pltpu.roll(west, 1, 1), 0.0) + jnp.where(high, east, 0.0)
        )
    sent2 = post(lines2, outbox2, inbox2, send2, recv2)

    for copy in shared1:
        copy.wait_recv()
    best = mine1[...]
    for d in range(len(first_peers)):
        best = jnp.maximum(best, gather1[d])
    mine2[...] = best
    shared2 = share(mine2, gather2, second_peers, msend2, mrecv2)

    spread(jump1)
    add_rows(rate1, jump1)

    def patch_up(c, _):
        rows = pl.ds(pl.multiple_of(c * ROWS, ROWS), ROWS)
        both = cols[rows, :]
        for f, p, m in pairs:
            side = pltpu.roll(both, n - (2 * m + 1), 1)
            rate1[f, p, rows, :] = rate1[f, p, rows, :] + jnp.where(edge, side, 0.0)
        return _

    lax.fori_loop(0, chunks, patch_up, 0, unroll=chunks)
    derive(rate1)
    interior(rate2)

    for copy in shared2:
        copy.wait_recv()
    for d in range(len(second_peers)):
        best = jnp.maximum(best, gather2[d])
    bound = jnp.max(best, axis=1, keepdims=True)
    step = jnp.broadcast_to(cfl_number / (bound * (n - 1)), (ROWS, n))
    half = 0.5 * step * step

    for copy in sent2:
        copy.wait_recv()
    jump2 = jumps(lines2, inbox2)
    spread(jump2)
    add_rows(rate2, jump2)
    for p in range(slots):
        live = count[0] > p

        def finish(c, _):
            rows = pl.ds(pl.multiple_of(c * ROWS, ROWS), ROWS)
            both = cols[rows, :]
            for f in range(comps):
                side = pltpu.roll(both, n - (2 * (p * 8 + f) + 1), 1)
                second = rate2[f, p, rows, :] + jnp.where(edge, side, 0.0)
                value = fld[f, p, rows, :] + step * rate1[f, p, rows, :] + half * second
                out_v[f, p, rows, :] = jnp.where(live, value, 0.0)
            return _

        lax.fori_loop(0, chunks, finish, 0, unroll=chunks)
    for copy in sent1 + sent2 + shared1 + shared2:
        copy.wait_send()


def shards(
    total, subs, fields, density, moduli, metric_diag, metric_cross, extension, count, connectivity
):
    comps, slots, n, _ = fields.shape
    group = max(g for g in range(1, total) if total % g == 0 and g * g <= total)
    inner, outer, _ = circulant(n, extension.shape[0])
    f32 = jnp.float32
    vmem = pl.BlockSpec(memory_space=pltpu.VMEM)
    smem = pl.BlockSpec(memory_space=pltpu.SMEM)
    hbm = pl.BlockSpec(memory_space=pltpu.HBM)
    state = pltpu.VMEM(fields.shape, f32)
    dma = pltpu.SemaphoreType.DMA
    boxed = pltpu.VMEM((4, slots, 8, n), f32)
    arrived = pltpu.VMEM((4 * slots, 8, n), f32)
    quotient = total // group
    return pl.pallas_call(
        functools.partial(kernel, total, subs, group),
        out_shape=pltpu.VMEM(fields.shape, f32),
        in_specs=[smem, smem] + [hbm] * 5 + [vmem] * 3,
        out_specs=vmem,
        scratch_shapes=[
            state,
            pltpu.VMEM(density.shape, f32),
            pltpu.VMEM(moduli.shape, f32),
            pltpu.VMEM(metric_diag.shape, f32),
            pltpu.VMEM(metric_cross.shape, f32),
            state, state, state, state,
            pltpu.VMEM((2 * n, 2 * n), jnp.bfloat16),
            pltpu.VMEM((2 * n, 2 * n), jnp.bfloat16),
            pltpu.VMEM((n, n), f32),
            pltpu.VMEM((n, n), f32),
            pltpu.VMEM((n, n), f32),
            pltpu.VMEM((slots * 4, 8, n), f32),
            pltpu.VMEM((slots * 4, 8, n), f32),
            boxed, boxed, arrived, arrived,
            pltpu.VMEM((1, n), f32),
            pltpu.VMEM((1, n), f32),
            pltpu.VMEM((group - 1, 1, n), f32),
            pltpu.VMEM((quotient - 1, 1, n), f32),
            dma((5,)),
            dma((4,)), dma((4,)), dma((4,)), dma((4,)),
            dma((group - 1,)), dma((group - 1,)), dma((quotient - 1,)), dma((quotient - 1,)),
        ],
        compiler_params=pltpu.CompilerParams(collective_id=0, has_side_effects=True),
    )(connectivity.T, count, fields, density, moduli, metric_diag, metric_cross, extension.T,
      jnp.asarray(inner), jnp.asarray(outer))


def solution(mesh):
    placed = (
        P(None, ("patch", "sub"), None, None),
        P(("patch", "sub"), None, None),
        P(None, ("patch", "sub"), None, None),
        P(None, ("patch", "sub"), None, None),
        P(None, ("patch", "sub"), None, None),
        P(),
        P(("patch", "sub")),
        P(("patch", "sub"), None),
    )
    total = mesh.shape["patch"] * mesh.shape["sub"]
    return jax.shard_map(
        functools.partial(shards, total, mesh.shape["sub"]),
        mesh=mesh,
        in_specs=placed,
        out_specs=P(None, ("patch", "sub"), None, None),
        check_vma=False,
    )
```

```python
import functools

import jax
import jax.numpy as jnp
import numpy as np
from jax import lax
from jax.experimental import pallas as pl
from jax.experimental.pallas import tpu as pltpu
from jax.sharding import PartitionSpec as P

MESH = pl.DeviceIdType.MESH
ROWS = 8
cfl_number = 0.5
penalty_weight = 0.5


def circulant(points, extra):
    length = points + extra
    half = (length - 1) // 2
    waves = np.arange(1, half + 1, dtype=np.float64)
    weights = waves * (2.0 * np.pi * (points - 1) / length)
    shifts = np.arange(length)
    phase = 2.0 * np.pi / length * (waves[:, None] * shifts[None, :] % length)
    kernel = -(2.0 / length) * np.sum(weights[:, None] * np.sin(phase), axis=0)
    at = (np.arange(points)[:, None] - np.arange(length)[None, :]) % length
    full = kernel[at].astype(np.float32)
    padded = -(-extra // ROWS) * ROWS
    outer = np.zeros((points, points), np.float32)
    outer[:, :extra] = full[:, points:]
    return full[:, :points], outer, padded


def split(x):
    hi = x.astype(jnp.bfloat16)
    lo = (x - hi.astype(jnp.float32)).astype(jnp.bfloat16)
    return hi, lo


def kernel(
    total, subs, group,
    conn, count, fields_hbm, density_hbm, moduli_hbm, diag_hbm, cross_hbm, ext, inner, outer,
    out_v,
    fld, den, mod, dia, cro, rate1, rate2, dxi, deta, left, right, ext_v, cols, trans,
    lines, lines2, outbox1, outbox2, inbox1, inbox2, mine1, mine2, gather1, gather2,
    load_sem, send1, recv1, send2, recv2, msend1, mrecv1, msend2, mrecv2,
):
    comps, slots, n, _ = fld.shape
    sides = slots * 4
    chunks = n // ROWS
    me = lax.axis_index("patch") * subs + lax.axis_index("sub")
    far = total // 2 + 1
    offsets = (1, total - 1, far, total - far)
    quotient = total // group
    rank = lax.rem(me, group)
    base = me - rank
    block = lax.div(me, group)

    def place(flat):
        return (lax.div(flat, subs), lax.rem(flat, subs))

    loads = [pltpu.make_async_copy(fields_hbm, fld, load_sem.at[0])]
    for at, (src, dst) in enumerate(
        ((density_hbm, den), (moduli_hbm, mod), (diag_hbm, dia), (cross_hbm, cro))
    ):
        loads.append(pltpu.make_async_copy(src, dst, load_sem.at[at + 1]))
    for load in loads:
        load.start()

    barrier = pltpu.get_barrier_semaphore()
    near = [lax.rem(me + off, total) for off in offsets]
    first_peers = [base + lax.rem(rank + d, group) for d in range(1, group)]
    second_peers = [lax.rem(block + d, quotient) * group + rank for d in range(1, quotient)]
    everyone = near + first_peers + second_peers
    for peer in everyone:
        pl.semaphore_signal(barrier, inc=1, device_id=place(peer), device_id_type=MESH)

    owner = [conn[0, s] for s in range(sides)]
    strip = [conn[1, s] for s in range(sides)]
    flip = [conn[2, s] for s in range(sides)]
    picks = []
    for peer in near:
        seen = jnp.int32(0)
        pick = [jnp.int32(0)] * slots
        for s in range(sides):
            hit = owner[s] == peer
            for k in range(slots):
                pick[k] = jnp.where(hit & (seen == k), s, pick[k])
            seen = seen + hit.astype(jnp.int32)
        picks.append(pick)
    box, local = [], []
    for s in range(sides):
        pos = jnp.int32(0)
        for t in range(sides):
            if t != s:
                pos = pos + ((owner[t] == owner[s]) & (strip[t] < strip[s])).astype(jnp.int32)
        pos = jnp.minimum(pos, slots - 1)
        at = pos
        for o, off in enumerate(offsets):
            at = jnp.where(owner[s] == lax.rem(me + total - off, total), o * slots + pos, at)
        box.append(at)
        local.append(owner[s] == me)

    lane = lax.broadcasted_iota(jnp.int32, (ROWS, n), 1)
    low, high = lane == 0, lane == n - 1
    edge = low | high
    pairs = [(f, p, p * 8 + f) for p in range(slots) for f in range(comps)]

    def collect(state, lines):
        def columns(c, _):
            rows = pl.ds(pl.multiple_of(c * ROWS, ROWS), ROWS)
            acc = jnp.zeros((ROWS, n), jnp.float32)
            for f, p, m in pairs:
                turned = pltpu.roll(state[f, p, rows, :], 2 * m + 1, 1)
                acc = jnp.where((lane == 2 * m) | (lane == 2 * m + 1), turned, acc)
            cols[rows, :] = acc
            return _

        lax.fori_loop(0, chunks, columns, 0, unroll=chunks)
        trans[...] = jnp.transpose(cols[...])
        for p in range(slots):
            lines[p * 4 + 2] = trans[pl.ds(p * 16 + 1, 8, stride=2), :]
            lines[p * 4 + 3] = trans[pl.ds(p * 16, 8, stride=2), :]
            for f in range(comps):
                lines[p * 4, pl.ds(f, 1)] = state[f, p, pl.ds(0, 1), :]
                lines[p * 4 + 1, pl.ds(f, 1)] = state[f, p, pl.ds(n - 1, 1), :]

    def post(lines, outbox, inbox, send, recv):
        for o in range(4):
            for k in range(slots):
                outbox[o, k] = lines[picks[o][k]]
        sent = []
        for o in range(4):
            copy = pltpu.make_async_remote_copy(
                src_ref=outbox.at[o],
                dst_ref=inbox.at[pl.ds(o * slots, slots)],
                send_sem=send.at[o],
                recv_sem=recv.at[o],
                device_id=place(near[o]),
                device_id_type=MESH,
            )
            copy.start()
            sent.append(copy)
        return sent

    def jumps(lines, inbox):
        found = []
        for s in range(sides):
            partner = jnp.where(local[s], lines[strip[s]], inbox[box[s]])
            index = jnp.where(flip[s] == 1, n - 1 - lane, lane)
            partner = jnp.take_along_axis(partner, index, axis=1)
            scale = jnp.where(owner[s] >= 0, penalty_weight * (n - 1), 0.0)
            found.append(scale * (partner - lines[s]))
        return found

    def spread(jump):
        for p in range(slots):
            trans[pl.ds(p * 16 + 1, 8, stride=2), :] = jump[p * 4 + 2]
            trans[pl.ds(p * 16, 8, stride=2), :] = jump[p * 4 + 3]
        cols[...] = jnp.transpose(trans[...])

    def derive(state):
        for f in range(comps):
            h0, l0 = split(state[f, 0])
            h1, l1 = split(state[f, 1])
            rows = jnp.concatenate(
                [jnp.concatenate([h0, l0], axis=1), jnp.concatenate([h1, l1], axis=1)], axis=0
            )
            eta = jnp.dot(rows, right[...], preferred_element_type=jnp.float32)
            both = eta[:, :n] + eta[:, n:]
            deta[f, 0] = both[:n]
            deta[f, 1] = both[n:]
            body = jnp.concatenate(
                [jnp.concatenate([h0, h1], axis=1), jnp.concatenate([l0, l1], axis=1)], axis=0
            )
            xi = jnp.dot(left[...], body, preferred_element_type=jnp.float32)
            both = xi[:n] + xi[n:]
            dxi[f, 0] = both[:, :n]
            dxi[f, 1] = both[:, n:]

    def interior(rate):
        for p in range(slots):

            def body(c, _):
                rows = pl.ds(pl.multiple_of(c * ROWS, ROWS), ROWS)
                xx, yy = dia[0, p, rows, :], dia[1, p, rows, :]
                xy, ex = cro[0, p, rows, :], cro[1, p, rows, :]
                lame, shear = mod[0, p, rows, :], mod[1, p, rows, :]
                inv = den[p, rows, :]
                stiff = lame + 2.0 * shear
                ax = [dxi[f, p, rows, :] for f in range(comps)]
                ay = [deta[f, p, rows, :] for f in range(comps)]
                gx = [xx * a + ex * b for a, b in zip(ax, ay)]
                gy = [xy * a + yy * b for a, b in zip(ax, ay)]
                rate[0, p, rows, :] = (gx[2] + gy[4]) * inv
                rate[1, p, rows, :] = (gx[4] + gy[3]) * inv
                rate[2, p, rows, :] = stiff * gx[0] + lame * gy[1]
                rate[3, p, rows, :] = lame * gx[0] + stiff * gy[1]
                rate[4, p, rows, :] = shear * (gy[0] + gx[1])
                return _

            lax.fori_loop(0, chunks, body, 0, unroll=chunks)

    def add_rows(rate, jump):
        for p in range(slots):
            for f in range(comps):
                for side, at in ((0, 0), (1, n - 1)):
                    spot = pl.ds(at, 1)
                    rate[f, p, spot, :] = rate[f, p, spot, :] + jump[p * 4 + side][f : f + 1]

    lines[...] = jnp.zeros_like(lines)
    lines2[...] = jnp.zeros_like(lines2)
    trans[...] = jnp.zeros_like(trans)
    loads[0].wait()
    collect(fld, lines)
    pl.semaphore_wait(barrier, len(everyone))
    sent1 = post(lines, outbox1, inbox1, send1, recv1)
    ext_v[...] = jnp.zeros_like(ext_v)
    twice, extra = ext.shape
    ext_v[pl.ds(0, twice), pl.ds(0, extra)] = ext[...]
    turned = pltpu.roll(ext_v[...], n - twice // 2, 0)
    matrix = inner[...] + lax.dot_general(
        outer[...],
        turned,
        (((1,), (1,)), ((), ())),
        precision=lax.Precision.HIGHEST,
        preferred_element_type=jnp.float32,
    )
    hi, lo = split(matrix)
    none = jnp.zeros_like(hi)
    left[...] = jnp.concatenate(
        [jnp.concatenate([hi, hi], axis=1), jnp.concatenate([lo, none], axis=1)], axis=0
    )
    hi, lo = split(jnp.transpose(matrix))
    right[...] = jnp.concatenate(
        [jnp.concatenate([hi, lo], axis=1), jnp.concatenate([hi, none], axis=1)], axis=0
    )
    derive(fld)

    for load in loads[1:]:
        load.wait()
    top = jnp.zeros((ROWS, n), jnp.float32)
    for p in range(slots):

        def speeds(c, top):
            rows = pl.ds(pl.multiple_of(c * ROWS, ROWS), ROWS)
            xx, yy = dia[0, p, rows, :], dia[1, p, rows, :]
            xy, ex = cro[0, p, rows, :], cro[1, p, rows, :]
            stiff = mod[0, p, rows, :] + 2.0 * mod[1, p, rows, :]
            inv = 1.0 / den[p, rows, :]
            den[p, rows, :] = inv
            speed = jnp.sqrt(stiff * inv) * (
                jnp.sqrt(xx * xx + xy * xy) + jnp.sqrt(ex * ex + yy * yy)
            )
            return jnp.maximum(top, speed)

        part = lax.fori_loop(
            0, chunks, speeds, jnp.zeros((ROWS, n), jnp.float32), unroll=chunks
        )
        top = jnp.maximum(top, jnp.where(count[0] > p, part, 0.0))

    def share(mine, gather, peers, send, recv):
        sent = []
        for d, peer in enumerate(peers):
            copy = pltpu.make_async_remote_copy(
                src_ref=mine,
                dst_ref=gather.at[d],
                send_sem=send.at[d],
                recv_sem=recv.at[d],
                device_id=place(peer),
                device_id_type=MESH,
            )
            copy.start()
            sent.append(copy)
        return sent

    mine1[...] = jnp.max(top, axis=0, keepdims=True)
    shared1 = share(mine1, gather1, first_peers, msend1, mrecv1)
    interior(rate1)

    collect(rate1, lines2)
    for copy in sent1:
        copy.wait_recv()
    jump1 = jumps(lines, inbox1)
    for p in range(slots):
        west, east, south, north = jump1[p * 4 : p * 4 + 4]
        lines2[p * 4] += (
            west + jnp.where(low, south, 0.0) + jnp.where(high, pltpu.roll(north, n - 1, 1), 0.0)
        )
        lines2[p * 4 + 1] += (
            east + jnp.where(low, pltpu.roll(south, 1, 1), 0.0) + jnp.where(high, north, 0.0)
        )
        lines2[p * 4 + 2] += (
            south + jnp.where(low, west, 0.0) + jnp.where(high, pltpu.roll(east, n - 1, 1), 0.0)
        )
        lines2[p * 4 + 3] += (
            north + jnp.where(low, pltpu.roll(west, 1, 1), 0.0) + jnp.where(high, east, 0.0)
        )
    sent2 = post(lines2, outbox2, inbox2, send2, recv2)

    for copy in shared1:
        copy.wait_recv()
    best = mine1[...]
    for d in range(len(first_peers)):
        best = jnp.maximum(best, gather1[d])
    mine2[...] = best
    shared2 = share(mine2, gather2, second_peers, msend2, mrecv2)

    spread(jump1)
    add_rows(rate1, jump1)

    def patch_up(c, _):
        rows = pl.ds(pl.multiple_of(c * ROWS, ROWS), ROWS)
        both = cols[rows, :]
        for f, p, m in pairs:
            side = pltpu.roll(both, n - (2 * m + 1), 1)
            rate1[f, p, rows, :] = rate1[f, p, rows, :] + jnp.where(edge, side, 0.0)
        return _

    lax.fori_loop(0, chunks, patch_up, 0, unroll=chunks)
    derive(rate1)
    interior(rate2)

    for copy in shared2:
        copy.wait_recv()
    for d in range(len(second_peers)):
        best = jnp.maximum(best, gather2[d])
    bound = jnp.max(best, axis=1, keepdims=True)
    step = jnp.broadcast_to(cfl_number / (bound * (n - 1)), (ROWS, n))
    half = 0.5 * step * step

    for copy in sent2:
        copy.wait_recv()
    jump2 = jumps(lines2, inbox2)
    spread(jump2)
    add_rows(rate2, jump2)
    for p in range(slots):
        live = count[0] > p

        def finish(c, _):
            rows = pl.ds(pl.multiple_of(c * ROWS, ROWS), ROWS)
            both = cols[rows, :]
            for f in range(comps):
                side = pltpu.roll(both, n - (2 * (p * 8 + f) + 1), 1)
                second = rate2[f, p, rows, :] + jnp.where(edge, side, 0.0)
                value = fld[f, p, rows, :] + step * rate1[f, p, rows, :] + half * second
                out_v[f, p, rows, :] = jnp.where(live, value, 0.0)
            return _

        lax.fori_loop(0, chunks, finish, 0, unroll=chunks)
    for copy in sent1 + sent2 + shared1 + shared2:
        copy.wait_send()


def shards(
    total, subs, fields, density, moduli, metric_diag, metric_cross, extension, count, connectivity
):
    comps, slots, n, _ = fields.shape
    group = max(g for g in range(1, total) if total % g == 0 and g * g <= total)
    inner, outer, _ = circulant(n, extension.shape[0])
    f32 = jnp.float32
    vmem = pl.BlockSpec(memory_space=pltpu.VMEM)
    smem = pl.BlockSpec(memory_space=pltpu.SMEM)
    hbm = pl.BlockSpec(memory_space=pltpu.HBM)
    state = pltpu.VMEM(fields.shape, f32)
    dma = pltpu.SemaphoreType.DMA
    boxed = pltpu.VMEM((4, slots, 8, n), f32)
    arrived = pltpu.VMEM((4 * slots, 8, n), f32)
    quotient = total // group
    return pl.pallas_call(
        functools.partial(kernel, total, subs, group),
        out_shape=pltpu.VMEM(fields.shape, f32),
        in_specs=[smem, smem] + [hbm] * 5 + [vmem] * 3,
        out_specs=vmem,
        scratch_shapes=[
            state,
            pltpu.VMEM(density.shape, f32),
            pltpu.VMEM(moduli.shape, f32),
            pltpu.VMEM(metric_diag.shape, f32),
            pltpu.VMEM(metric_cross.shape, f32),
            state, state, state, state,
            pltpu.VMEM((2 * n, 2 * n), jnp.bfloat16),
            pltpu.VMEM((2 * n, 2 * n), jnp.bfloat16),
            pltpu.VMEM((n, n), f32),
            pltpu.VMEM((n, n), f32),
            pltpu.VMEM((n, n), f32),
            pltpu.VMEM((slots * 4, 8, n), f32),
            pltpu.VMEM((slots * 4, 8, n), f32),
            boxed, boxed, arrived, arrived,
            pltpu.VMEM((1, n), f32),
            pltpu.VMEM((1, n), f32),
            pltpu.VMEM((group - 1, 1, n), f32),
            pltpu.VMEM((quotient - 1, 1, n), f32),
            dma((5,)),
            dma((4,)), dma((4,)), dma((4,)), dma((4,)),
            dma((group - 1,)), dma((group - 1,)), dma((quotient - 1,)), dma((quotient - 1,)),
        ],
        compiler_params=pltpu.CompilerParams(collective_id=0, has_side_effects=True),
    )(connectivity.T, count, fields, density, moduli, metric_diag, metric_cross, extension.T,
      jnp.asarray(inner), jnp.asarray(outer))


def solution(mesh):
    placed = (
        P(None, ("patch", "sub"), None, None),
        P(("patch", "sub"), None, None),
        P(None, ("patch", "sub"), None, None),
        P(None, ("patch", "sub"), None, None),
        P(None, ("patch", "sub"), None, None),
        P(),
        P(("patch", "sub")),
        P(("patch", "sub"), None),
    )
    total = mesh.shape["patch"] * mesh.shape["sub"]
    return jax.shard_map(
        functools.partial(shards, total, mesh.shape["sub"]),
        mesh=mesh,
        in_specs=placed,
        out_specs=P(None, ("patch", "sub"), None, None),
        check_vma=False,
    )
```
